256 devices in a mesh: groups: 4 (over x, y), req: 64 (over z, core).
Axes of the slice: x: 2, y: 2, z: 32, core: 2. Of those that a mesh axis runs over, the one named last changes fastest.
The devices are a block of a 4x8x32 slice.
Arguments:
- cache_states: bfloat16 [256, 16, 8192], P(('groups', 'req')), parts along dimension 0, may hold values from -6 to 6
- pool_keys: bfloat16 [4096, 64, 512], P(('groups', 'req')), parts along dimension 0, may hold values from -64 to 64
- pool_values: bfloat16 [4096, 64, 512], P(('groups', 'req')), parts along dimension 0, may hold values from -6 to 6
- slot_prefix: int32 [256], P('groups'), parts along dimension 0, may hold values from 0 to 63, each once
- page_table: int32 [256, 16], P('groups'), parts along dimension 0, may hold values from 0 to 15, each once within a row
- prefix_id: int32 [256], P('groups'), parts along dimension 0, may hold values from 0 to 63
- lengths: int32 [256], P(('groups', 'req')), parts along dimension 0, may hold values from 32 to 128, as said below
- queries: bfloat16 [32768, 4096], P(('groups', 'req')), parts along dimension 0, may hold values from -64 to 64
- suffix_keys: bfloat16 [32768, 512], P(('groups', 'req')), parts along dimension 0, may hold values from -6 to 6
- suffix_values: bfloat16 [32768, 512], P(('groups', 'req')), parts along dimension 0, may hold values from -6 to 6
- u_in: bfloat16 [32768, 8192], P(('groups', 'req')), parts along dimension 0, may hold values from -6 to 6
- dt_raw: bfloat16 [32768, 8192], P(('groups', 'req')), parts along dimension 0, may hold values from -3 to 3
- bc_in: float32 [256, 32, 128], P(('groups', 'req')), parts along dimension 0, may hold values from -6 to 6
- a_log: float32 [16, 8192], replicated, may hold values from 0 to 2.77
- dt_bias: float32 [8192], replicated, may hold values from -7 to -2.3
- d_skip: float32 [8192], replicated, may hold values from 0.5 to 1.5
Outputs:
- mamba_out: bfloat16 [32768, 8192], P(('groups', 'req')), parts along dimension 0
- attn_out: bfloat16 [32768, 4096], P(('groups', 'req')), parts along dimension 0
- final_state: float32 [256, 16, 8192], P(('groups', 'req')), parts along dimension 0
The draws below stay inside these ranges and needn't reach their ends.
There are 4 independent parts, one for each index of `groups`. The reference program is written for one: setup_inputs(seed, part) draws one part's arguments, and reference() takes and returns one part's arrays. A program takes and returns all parts, laid end to end along the dimension named above; an argument that names none is the same for every part. Nothing has to cross between parts.
Inputs may be any that keep to these rules, and one draw needn't show every extreme that they name: `slot_prefix`: each prefix is held by exactly one slot. `page_table`: each row is a permutation of the local pages. `lengths`: some request has exactly 128 live tokens.
All inputs are finite; a program needn't handle non-finite values.
Results may differ from the reference program's by a relative error of at most 0.0049.
Values may be sent and summed in bfloat16 or wider, within the bound.
No kernel may reach another device: no remote copies, remote signals or barrier semaphores. Data moves between devices by JAX's collectives and lax.ppermute only.
A program may use at most 128 MiB of HBM per device.

```python
import math
import jax
import jax.numpy as jnp
import numpy as np
from jax import lax

DW = 8192
NSTATE = 16
QH = 32
KH = 4
HD = 128
PAGE = 64
L = 128
PAGES = 16
REQS = 64
NPRE = 64


def draw_queries(key, part):
    shape = (REQS * L, QH * HD)
    base = jax.random.truncated_normal(jax.random.fold_in(key, 12), -6.0, 6.0, shape, jnp.float32)
    return base.astype(jnp.bfloat16)


def draw_pool_keys(key, part):
    shape = (NPRE * PAGES, PAGE, KH * HD)
    base = jax.random.truncated_normal(jax.random.fold_in(key, 14), -6.0, 6.0, shape, jnp.float32)
    return base.astype(jnp.bfloat16)


def draw_lengths(key, part):
    counts = jax.random.randint(jax.random.fold_in(key, 21), (REQS,), L // 4, L + 1, jnp.int32)
    chosen = jax.random.randint(jax.random.fold_in(key, 22), (), 0, REQS, jnp.int32)
    return counts.at[chosen].set(L)


def plant(values, key, low, largest):
    shape = values.shape
    index_at = [jax.random.randint(jax.random.fold_in(key, axis), (), 0, shape[axis]) for axis in range(len(shape))]
    values = values.at[tuple(index_at)].set(low)
    longest = shape.index(max(shape))
    index_at[longest] = (index_at[longest] + 1) % shape[longest]
    return values.at[tuple(index_at)].set(largest)


def block_levels(key, extent, cuts, smallest, top_value):
    level, own = 1.0, jax.random.fold_in(key, 6)
    for dim, shards_of in cuts:
        steps = jnp.exp(jax.random.uniform(jax.random.fold_in(own, dim), (shards_of,), jnp.float32, smallest / len(cuts), top_value / len(cuts)))
        level = level * jnp.repeat(steps, extent[dim] // shards_of).reshape([-1 if axis == dim else 1 for axis in range(len(extent))])
    return level


def cumulative_ranks(number_of, slope):
    portions = [(1 << 20) // math.isqrt(standing ** slope) + 1 for standing in range(1, number_of + 1)]
    spread = 1 + sum(portions) // (1 << 30)
    return np.cumsum(np.array([max(1, weight // spread) for weight in portions]))


def skewed_ids(rng, extent, amount, skew):
    table = cumulative_ranks(amount, skew)
    pick = jax.random.randint(jax.random.fold_in(rng, 1), extent, 0, int(table[amount - 1]))
    rank = jnp.searchsorted(jnp.asarray(table, jnp.int32), pick, side="right")
    return jax.random.permutation(jax.random.fold_in(rng, 2), amount)[rank].astype(jnp.int32)


def gaussian(rng, shape, deviation, bound, cuts=(), kind=jnp.bfloat16):
    drawn = jax.random.normal(rng, shape, jnp.float32) * deviation
    if len(cuts) > 0:
        drawn = block_levels(rng, shape, cuts, -0.22, 0.18) * drawn
    return jnp.clip(drawn, min=-bound, max=bound).astype(kind)


def setup_inputs(seed: int = 0, part: int = 0) -> dict:
    keys = jax.random.split(jax.random.key(seed), 17)
    part_splits = jax.random.split(jax.random.fold_in(keys[16], part), 17)
    cache_states = gaussian(part_splits[0], (NPRE, NSTATE, DW), 1.0, 6.0, ((0, 64),))
    pool_keys = draw_pool_keys(jax.random.fold_in(jax.random.fold_in(keys[16], part), 71), part)
    pool_values = gaussian(part_splits[2], (NPRE * PAGES, PAGE, KH * HD), 1.0, 6.0, ((0, 64),))
    slot_prefix = jax.random.permutation(part_splits[3], NPRE).astype(jnp.int32)
    page_table = jax.vmap(lambda own: jax.random.permutation(own, PAGES))(jax.random.split(part_splits[4], NPRE)).reshape((NPRE, PAGES)).astype(jnp.int32)
    prefix_id = plant(skewed_ids(part_splits[5], (REQS,), NPRE, 2), jax.random.fold_in(part_splits[5], 3), 0, NPRE - 1).astype(jnp.int32)
    lengths = draw_lengths(jax.random.fold_in(jax.random.fold_in(keys[16], part), 71), part)
    queries = draw_queries(jax.random.fold_in(jax.random.fold_in(keys[16], part), 71), part)
    suffix_keys = gaussian(part_splits[8], (REQS * L, KH * HD), 1.0, 6.0, ((0, 64),))
    suffix_values = gaussian(part_splits[9], (REQS * L, KH * HD), 1.0, 6.0, ((0, 64),))
    u_in = gaussian(part_splits[10], (REQS * L, DW), 1.0, 6.0, ((0, 64),))
    dt_raw = gaussian(part_splits[11], (REQS * L, DW), 0.5, 3.0, ((0, 64),))
    bc_in = gaussian(part_splits[12], (REQS, 2 * NSTATE, L), 1.0, 6.0, ((0, 64),), jnp.float32)
    a_log = jnp.clip(jax.random.uniform(keys[13], (NSTATE, DW), jnp.float32, 0.0, 2.77), 0.0, 2.77)
    dt_bias = jnp.clip(jax.random.uniform(keys[14], (DW,), jnp.float32, -7.0, -2.3), -7.0, -2.3)
    d_skip = jnp.clip(jax.random.uniform(keys[15], (DW,), jnp.float32, 0.5, 1.5), 0.5, 1.5)
    return {"cache_states": cache_states, "pool_keys": pool_keys, "pool_values": pool_values, "slot_prefix": slot_prefix, "page_table": page_table, "prefix_id": prefix_id, "lengths": lengths, "queries": queries, "suffix_keys": suffix_keys, "suffix_values": suffix_values, "u_in": u_in, "dt_raw": dt_raw, "bc_in": bc_in, "a_log": a_log, "dt_bias": dt_bias, "d_skip": d_skip}


def scan_tokens(start_state, u_rows, dt_rows, bc_rows, a_log, dt_bias, d_skip, length):
    rates = -jnp.exp(a_log)
    position = jnp.arange(u_rows.shape[0], dtype=jnp.int32)
    live_rows = (position < length).astype(jnp.float32)[:, None]
    deltas = jax.nn.softplus(dt_rows.astype(jnp.float32) + dt_bias[None, :]) * live_rows
    inputs = u_rows.astype(jnp.float32)

    def advance(carried, sliced):
        delta_row, input_row, b_col, c_col = sliced
        carried = jnp.exp(delta_row[None, :] * rates) * carried + (delta_row * input_row)[None, :] * b_col[:, None]
        return (carried, lax.optimization_barrier(jnp.sum(c_col[:, None] * carried, axis=0)))
    last_state, scanned = lax.scan(advance, start_state, (deltas, inputs, jnp.transpose(bc_rows[:NSTATE]), jnp.transpose(bc_rows[NSTATE:])))
    outputs = scanned + d_skip[None, :] * inputs
    return ((outputs * live_rows).astype(jnp.bfloat16), last_state)

def attend(query_rows, prefix_keys, prefix_values, suffix_keys, suffix_values, length):
    row_count = query_rows.shape[0]
    q_group = QH // KH
    prefix_len = prefix_keys.shape[0]
    keys_all = jnp.concatenate([prefix_keys, suffix_keys], axis=0)
    values_all = jnp.concatenate([prefix_values, suffix_values], axis=0)
    position = jnp.arange(row_count, dtype=jnp.int32)
    key_pos = jnp.arange(prefix_len + row_count, dtype=jnp.int32) - prefix_len
    visible = (key_pos[None, :] <= position[:, None]) & (key_pos[None, :] > position[:, None] - prefix_len)
    score_scale = 1.0 / math.sqrt(HD)
    pieces = []
    for kv_head in range(KH):
        q_block = query_rows[:, kv_head * q_group * HD:(kv_head + 1) * q_group * HD].reshape(row_count * q_group, HD)
        k_block = keys_all[:, kv_head * HD:(kv_head + 1) * HD]
        scores = lax.dot_general(q_block, k_block, (((1,), (1,)), ((), ())), preferred_element_type=jnp.float32) * score_scale
        scores = scores.reshape(row_count, q_group, -1)
        scores = jnp.where(visible[:, None, :], scores, -1e+30)
        highest = lax.optimization_barrier(jnp.max(scores, axis=2, keepdims=True))
        exponent = jnp.exp(scores - highest)
        totals = lax.optimization_barrier(jnp.sum(exponent, axis=2, keepdims=True))
        weights = (exponent / totals).astype(jnp.bfloat16).reshape(row_count * q_group, -1)
        mixed_rows = jnp.dot(weights, values_all[:, kv_head * HD:(kv_head + 1) * HD], preferred_element_type=jnp.float32)
        pieces.append(mixed_rows.astype(jnp.bfloat16).reshape(row_count, q_group * HD))
    result = jnp.concatenate(pieces, axis=1)
    live_rows = (position < length)[:, None]
    return jnp.where(live_rows, result, jnp.zeros_like(result))

def reference(cache_states, pool_keys, pool_values, slot_prefix, page_table, prefix_id, lengths, queries, suffix_keys, suffix_values, u_in, dt_raw, bc_in, a_log, dt_bias, d_skip):
    slot_count = slot_prefix.shape[0]
    page_count = page_table.shape[1]
    matches = (slot_prefix[None, :] == prefix_id[:, None]).astype(jnp.int32)
    source = lax.optimization_barrier(jnp.sum(matches * jnp.arange(slot_count, dtype=jnp.int32)[None, :], axis=1)).astype(jnp.int32)

    def one_request(request):
        owner_slot = source[request]
        prefix = prefix_id[request]
        pool_rows = (owner_slot * page_count + page_table[prefix]).astype(jnp.int32)
        prefix_keys = jnp.take(pool_keys, pool_rows, axis=0).reshape(-1, KH * HD)
        prefix_values = jnp.take(pool_values, pool_rows, axis=0).reshape(-1, KH * HD)
        start_state = cache_states[owner_slot].astype(jnp.float32)
        first_row = (request * L).astype(jnp.int32)
        query_rows = lax.dynamic_slice_in_dim(queries, first_row, L, 0)
        key_rows = lax.dynamic_slice_in_dim(suffix_keys, first_row, L, 0)
        value_rows = lax.dynamic_slice_in_dim(suffix_values, first_row, L, 0)
        u_rows = lax.dynamic_slice_in_dim(u_in, first_row, L, 0)
        dt_rows = lax.dynamic_slice_in_dim(dt_raw, first_row, L, 0)
        length = lengths[request]
        mamba_rows, last_state = scan_tokens(start_state, u_rows, dt_rows, bc_in[request], a_log, dt_bias, d_skip, length)
        attn_rows = attend(query_rows, prefix_keys, prefix_values, key_rows, value_rows, length)
        return (mamba_rows, attn_rows, last_state)
    mamba_all, attn_all, states = lax.map(one_request, jnp.arange(REQS, dtype=jnp.int32))
    return (mamba_all.reshape(REQS * L, DW), attn_all.reshape(REQS * L, QH * HD), states)
```

```python
import functools
import math

import jax
import jax.numpy as jnp
from jax import lax
from jax.experimental import pallas as pl
from jax.experimental.pallas import tpu as pltpu
from jax.sharding import PartitionSpec as P

QH = 32
KH = 4
HD = 128

LANES = 128
SUB = 8
CHUNKS = 2
CHANNELS = SUB * LANES
LOG2E = math.log2(math.e)


def scan_kernel(length_ref, h0_ref, u_ref, dt_ref, b_ref, c_ref, a_ref, bias_ref, skip_ref, out_ref, last_ref,
                d_scr, x_scr, y_scr, h_scr, r_scr):
    tokens = u_ref.shape[0]
    nstate = a_ref.shape[0]
    length = length_ref[0]
    for n0 in range(0, nstate, SUB):
        for s in range(SUB):
            cols = pl.ds(s * LANES, LANES)
            rows = pl.ds(n0 * SUB + s, SUB, stride=SUB)
            r_scr[rows, :] = -jnp.exp(a_ref[n0:n0 + SUB, cols]) * LOG2E
    for s in range(SUB):
        first = h0_ref[:, s * LANES:(s + 1) * LANES].astype(jnp.float32)
        for n0 in range(0, nstate, SUB):
            h_scr[pl.ds(n0 * SUB + s, SUB, stride=SUB), :] = first[n0:n0 + SUB]

    def spread(k, carry):
        t0 = pl.multiple_of(k * 16, 16)
        live = (lax.broadcasted_iota(jnp.int32, (16, LANES), 0) + t0 < length).astype(jnp.float32)
        for s in range(SUB):
            cols = pl.ds(s * LANES, LANES)
            v = dt_ref[pl.ds(t0, 16), cols].astype(jnp.float32) + bias_ref[:, cols]
            delta = (jnp.maximum(v, 0.0) + jnp.log1p(jnp.exp(-jnp.abs(v)))) * live
            x = delta * u_ref[pl.ds(t0, 16), cols].astype(jnp.float32)
            for half in range(2):
                rows = pl.ds((t0 + half * SUB) * SUB + s, SUB, stride=SUB)
                d_scr[rows, :] = delta[half * SUB:(half + 1) * SUB]
                x_scr[rows, :] = x[half * SUB:(half + 1) * SUB]
        return carry

    lax.fori_loop(0, tokens // 16, spread, 0)

    def advance(t, h):
        row = pl.ds(pl.multiple_of(t * SUB, SUB), SUB)
        d = d_scr[row, :]
        x = x_scr[row, :]
        new = []
        sums = [None, None]
        for n in range(nstate):
            b = b_ref[pl.ds(t * nstate + n, 1), :]
            c = c_ref[pl.ds(t * nstate + n, 1), :]
            g = jnp.exp2(d * r_scr[n * SUB:(n + 1) * SUB, :]) * h[n] + x * b
            new.append(g)
            term = g * c
            sums[n % 2] = term if sums[n % 2] is None else sums[n % 2] + term
        y_scr[row, :] = sums[0] + sums[1]
        return tuple(new)

    h = lax.fori_loop(0, tokens, advance, tuple(h_scr[n * SUB:(n + 1) * SUB, :] for n in range(nstate)), unroll=2)
    for n in range(nstate):
        h_scr[n * SUB:(n + 1) * SUB, :] = h[n]
    for n0 in range(0, nstate, SUB):
        for s in range(SUB):
            last_ref[n0:n0 + SUB, s * LANES:(s + 1) * LANES] = h_scr[pl.ds(n0 * SUB + s, SUB, stride=SUB), :]

    def gather(k, carry):
        t0 = pl.multiple_of(k * 16, 16)
        live = lax.broadcasted_iota(jnp.int32, (16, LANES), 0) + t0 < length
        for s in range(SUB):
            cols = pl.ds(s * LANES, LANES)
            y = jnp.concatenate(
                [y_scr[pl.ds((t0 + half * SUB) * SUB + s, SUB, stride=SUB), :] for half in range(2)], axis=0)
            y = y + skip_ref[:, cols] * u_ref[pl.ds(t0, 16), cols].astype(jnp.float32)
            out_ref[pl.ds(t0, 16), cols] = jnp.where(live, y, 0.0).astype(jnp.bfloat16)
        return carry

    lax.fori_loop(0, tokens // 16, gather, 0)


def selective_scan(start_state, u_rows, dt_rows, bc_rows, a_log, dt_bias, d_skip, length):
    tokens, width = u_rows.shape
    nstate = a_log.shape[0]
    splat = [
        jnp.broadcast_to(jnp.transpose(half).reshape(-1, 1), (tokens * nstate, LANES))
        for half in (bc_rows[:nstate], bc_rows[nstate:])
    ]
    part = lambda rows: pl.BlockSpec((rows, CHANNELS), lambda i, *_: (0, i))
    whole = pl.BlockSpec((tokens * nstate, LANES), lambda i, *_: (0, 0))
    work = tokens * nstate * width
    return pl.pallas_call(
        scan_kernel,
        grid_spec=pltpu.PrefetchScalarGridSpec(
            num_scalar_prefetch=1,
            grid=(width // CHANNELS,),
            in_specs=[part(nstate), part(tokens), part(tokens), whole, whole, part(nstate), part(1), part(1)],
            out_specs=[part(tokens), part(nstate)],
            scratch_shapes=[pltpu.VMEM((tokens * SUB, LANES), jnp.float32)] * 3
            + [pltpu.VMEM((nstate * SUB, LANES), jnp.float32)] * 2,
        ),
        out_shape=[
            jax.ShapeDtypeStruct((tokens, width), jnp.bfloat16),
            jax.ShapeDtypeStruct((nstate, width), jnp.float32),
        ],
        cost_estimate=pl.CostEstimate(flops=7 * work, bytes_accessed=10 * tokens * width, transcendentals=work),
        name="selective_scan",
    )(length, start_state, u_rows, dt_rows, splat[0], splat[1], a_log, dt_bias[None], d_skip[None])


def attend_kernel(side_ref, order_ref, length_ref, keep_ref, got_ref, sk_ref, sv_ref, q_ref, out_ref,
                  k_scr, v_scr, sems, *, page, skip):
    tokens = q_ref.shape[0]
    pages = order_ref.shape[0]
    prefix = pages * page
    head = pl.program_id(0)
    group = q_ref.shape[1] // HD

    def copies(k_src, v_src):
        made = []
        for k in range(pages):
            src = pl.ds(pl.multiple_of(skip + order_ref[k] * page, page), page)
            dst = pl.ds(k * page, page)
            made.append(pltpu.make_async_copy(k_src.at[src], k_scr.at[dst], sems.at[2 * k]))
            made.append(pltpu.make_async_copy(v_src.at[src], v_scr.at[dst], sems.at[2 * k + 1]))
        tail = pl.ds(prefix, tokens)
        made.append(pltpu.make_async_copy(sk_ref, k_scr.at[tail], sems.at[2 * pages]))
        made.append(pltpu.make_async_copy(sv_ref, v_scr.at[tail], sems.at[2 * pages + 1]))
        for c in made:
            c.start()
        for c in made:
            c.wait()

    @pl.when((head == 0) & (side_ref[0] == 0))
    def _():
        copies(keep_ref, got_ref)

    @pl.when((head == 0) & (side_ref[0] != 0))
    def _():
        copies(got_ref, keep_ref)

    cols = pl.ds(pl.multiple_of(head * HD, HD), HD)
    keys = k_scr[:, cols]
    values = v_scr[:, cols]
    t = lax.broadcasted_iota(jnp.int32, (tokens, tokens), 0)
    p = lax.broadcasted_iota(jnp.int32, (tokens, tokens), 1)
    early = jnp.concatenate([p > t] * 2, axis=0)
    late = jnp.concatenate([p <= t] * 2, axis=0)
    live = lax.broadcasted_iota(jnp.int32, (tokens, HD), 0) < length_ref[0]
    scale = 1.0 / math.sqrt(HD)
    for j in range(0, group, 2):
        q = jnp.concatenate([q_ref[:, (j + i) * HD:(j + i + 1) * HD] for i in range(2)], axis=0)
        scores = lax.dot_general(q, keys, (((1,), (1,)), ((), ())), preferred_element_type=jnp.float32) * scale
        scores = jnp.concatenate(
            [
                jnp.where(early, scores[:, :tokens], -1e30),
                scores[:, tokens:prefix],
                jnp.where(late, scores[:, prefix:], -1e30),
            ],
            axis=1,
        )
        e = jnp.exp(scores - jnp.max(scores, axis=1, keepdims=True))
        weights = (e * (1.0 / jnp.sum(e, axis=1, keepdims=True))).astype(jnp.bfloat16)
        mixed = jnp.dot(weights, values, preferred_element_type=jnp.float32)
        for i in range(2):
            out_ref[:, (j + i) * HD:(j + i + 1) * HD] = jnp.where(
                live, mixed[i * tokens:(i + 1) * tokens], 0.0).astype(jnp.bfloat16)


def attend(queries, keep, got, order, side, suffix_keys, suffix_values, length, page):
    tokens, width = queries.shape
    pages = order.shape[0]
    kv_width = suffix_keys.shape[1]
    rows = pages * page + tokens
    anywhere = pl.BlockSpec(memory_space=pl.ANY)
    heads = pl.BlockSpec((tokens, width // KH), lambda i, *_: (0, i))
    return pl.pallas_call(
        functools.partial(attend_kernel, page=page, skip=keep.shape[0] - pages * page),
        grid_spec=pltpu.PrefetchScalarGridSpec(
            num_scalar_prefetch=3,
            grid=(KH,),
            in_specs=[anywhere] * 4 + [heads],
            out_specs=heads,
            scratch_shapes=[
                pltpu.VMEM((rows, kv_width), jnp.bfloat16),
                pltpu.VMEM((rows, kv_width), jnp.bfloat16),
                pltpu.SemaphoreType.DMA((2 * pages + 2,)),
            ],
        ),
        out_shape=jax.ShapeDtypeStruct((tokens, width), jnp.bfloat16),
        cost_estimate=pl.CostEstimate(
            flops=4 * tokens * width * rows, bytes_accessed=4 * tokens * width, transcendentals=tokens * QH * rows),
        name="attend",
    )(side, order, length, keep, got, suffix_keys, suffix_values, queries)


def fill_kernel(first_ref, a_ref, b_ref, store_ref, sems):
    first = first_ref[0]
    made = []
    for i, src in enumerate((a_ref, b_ref)):
        for k in range(CHUNKS):
            made.append(pltpu.make_async_copy(
                src.at[k], store_ref.at[first + i * CHUNKS + k], sems.at[i * CHUNKS + k]))
    for c in made:
        c.start()
    for c in made:
        c.wait()


def new_store(first, a, b, count):
    chunk = a.shape[1:]
    return pl.pallas_call(
        fill_kernel,
        grid_spec=pltpu.PrefetchScalarGridSpec(
            num_scalar_prefetch=1,
            grid=(1,),
            in_specs=[pl.BlockSpec(a.shape, lambda i, *_: (0, 0, 0))] * 2,
            out_specs=pl.BlockSpec(memory_space=pl.ANY),
            scratch_shapes=[pltpu.SemaphoreType.DMA((2 * CHUNKS,))],
        ),
        out_shape=jax.ShapeDtypeStruct((count,) + chunk, jnp.bfloat16),
        name="new_store",
    )(first, a, b)


def relay(store, source, chip, ring, slots):
    forward = [(i, (i + 2) % (2 * ring)) for i in range(2 * ring)]
    backward = [(i, (i - 2) % (2 * ring)) for i in range(2 * ring)]
    slot = jnp.arange(slots, dtype=jnp.int32)
    home = slot // 2
    place = jnp.arange(ring, dtype=jnp.int32)
    away = jnp.mod(place[:, None].repeat(2, 1).reshape(-1)[:, None] - home[None, :], ring)
    wanted = source[:, None] == slot[None, :]
    near = away <= ring // 2
    reach = jnp.stack([
        jnp.max(jnp.where(wanted & near, away, 0), axis=0),
        jnp.max(jnp.where(wanted & ~near, ring - away, 0), axis=0),
    ])
    gone = jnp.stack([jnp.mod(place[:, None] - home[None, :], ring), jnp.mod(home[None, :] - place[:, None], ring)])
    ahead = jnp.maximum(reach[:, None, :] - gone, 0)
    waiting = jnp.where((gone == 0) & (ahead > 0), CHUNKS, 0)
    rank = ahead * slots + slot[None, None, :]
    trash = slots * CHUNKS

    def plan(waiting, sent):
        urgent = jnp.where(waiting > 0, rank, 0)
        best = jnp.max(urgent, axis=2)
        chosen = ((urgent == best[:, :, None]) & (waiting > 0)).astype(jnp.int32)
        index = jnp.mod(best, slots) * CHUNKS + jnp.sum(chosen * sent, axis=2)
        index = jnp.where(best > 0, index, trash)
        arrived = jnp.stack([jnp.roll(chosen[0], 1, axis=0), jnp.roll(chosen[1], -1, axis=0)])
        took = jnp.stack([jnp.roll(index[0], 1), jnp.roll(index[1], -1)])
        mine = (place == chip).astype(jnp.int32)[None, :]
        gives = jnp.sum(index * mine, axis=1)
        takes = jnp.sum(took * mine, axis=1)
        busy = jnp.max(best) > 0
        return waiting - chosen + jnp.where(ahead > 0, arrived, 0), sent + chosen, gives, takes, busy

    def body(carry):
        store, waiting, sent, gives, takes, _ = carry
        out = [lax.dynamic_index_in_dim(store, gives[way], 0, keepdims=False) for way in range(2)]
        out = lax.optimization_barrier(tuple(out))
        right = lax.ppermute(out[0], "req", forward)
        left = lax.ppermute(out[1], "req", backward)
        planned = plan(waiting, sent)
        right, left, planned = lax.optimization_barrier((right, left, planned))
        store = lax.dynamic_update_index_in_dim(store, right, takes[0], 0)
        store = lax.dynamic_update_index_in_dim(store, left, takes[1], 0)
        waiting, sent, gives, then, busy = planned
        return store, waiting, sent, gives, then, busy

    start = (store,) + plan(waiting, jnp.zeros_like(waiting))
    return lax.while_loop(lambda carry: carry[5], body, start)[0]


def local(
    cache_states,
    pool_keys,
    pool_values,
    slot_prefix,
    page_table,
    prefix_id,
    lengths,
    queries,
    suffix_keys,
    suffix_values,
    u_in,
    dt_raw,
    bc_in,
    a_log,
    dt_bias,
    d_skip,
):
    me = lax.axis_index("req")
    side = jnp.mod(me, 2)
    chip = me // 2
    slots = slot_prefix.shape[0]
    ring = slots // 2
    swap = [(i, i ^ 1) for i in range(slots)]
    matches = (slot_prefix[None, :] == prefix_id[:, None]).astype(jnp.int32)
    source = jnp.sum(matches * jnp.arange(slots, dtype=jnp.int32)[None, :], axis=1)

    pages, page, kv_width = pool_keys.shape
    nstate, width = a_log.shape
    half = nstate // 2
    keys = pool_keys.reshape(pages * page, kv_width)
    values = pool_values.reshape(pages * page, kv_width)
    state = cache_states[0].reshape(2, half, width // kv_width, kv_width).transpose(0, 2, 1, 3)
    state = state.reshape(2, half * width // kv_width, kv_width)
    pack = lambda k: jnp.concatenate([state[k], (keys, values)[k]], axis=0).reshape(CHUNKS, -1, kv_width)
    key_half, value_half = pack(0), pack(1)
    mine = jnp.where(side == 0, key_half, value_half)
    theirs = lax.ppermute(jnp.where(side == 0, value_half, key_half), "req", swap)
    low = jnp.where(side == 0, mine, theirs)
    high = jnp.where(side == 0, theirs, mine)
    store = new_store((chip * 2 * CHUNKS)[None], low, high, slots * CHUNKS + 1)
    store = relay(store, source, chip, ring, slots)

    take = lambda r: lax.dynamic_slice_in_dim(store, source[r] * CHUNKS, CHUNKS, 0).reshape(-1, kv_width)
    keep = take(me)
    got = lax.ppermute(take(me + 1 - 2 * side), "req", swap)
    state_rows = half * width // kv_width
    pieces = (keep[:state_rows], got[:state_rows])
    spread = lambda a: a.reshape(width // kv_width, half, kv_width).transpose(1, 0, 2).reshape(half, width)
    start_state = jnp.concatenate(
        [spread(jnp.where(side == 0, pieces[k], pieces[1 - k])) for k in range(2)], axis=0)
    order = page_table[prefix_id[me]]
    mamba_out, last_state = selective_scan(start_state, u_in, dt_raw, bc_in[0], a_log, dt_bias, d_skip, lengths)
    attn_out = attend(queries, keep, got, order, side[None], suffix_keys, suffix_values, lengths, page)
    return (mamba_out, attn_out, last_state[None])


def solution(mesh):
    placed = (
        P(("groups", "req"), None, None),
        P(("groups", "req"), None, None),
        P(("groups", "req"), None, None),
        P("groups"),
        P("groups", None),
        P("groups"),
        P(("groups", "req")),
        P(("groups", "req"), None),
        P(("groups", "req"), None),
        P(("groups", "req"), None),
        P(("groups", "req"), None),
        P(("groups", "req"), None),
        P(("groups", "req"), None, None),
        P(),
        P(),
        P(),
    )
    return jax.shard_map(
        local,
        mesh=mesh,
        in_specs=placed,
        out_specs=(
            P(("groups", "req"), None),
            P(("groups", "req"), None),
            P(("groups", "req"), None, None),
        ),
        check_vma=False,
    )
```

```python
import functools
import math

import jax
import jax.numpy as jnp
from jax import lax
from jax.experimental import pallas as pl
from jax.experimental.pallas import tpu as pltpu
from jax.sharding import PartitionSpec as P

QH = 32
KH = 4
HD = 128

LANES = 128
SUB = 8
CHUNKS = 2
STREAMS = 2
FIRST = 8
DEPTH = 4
CHANNELS = SUB * LANES
LOG2E = math.log2(math.e)


def prepare_kernel(length_ref, u_ref, dt_ref, a_ref, bias_ref, d_ref, x_ref, r_ref):
    tokens = u_ref.shape[0]
    nstate = a_ref.shape[0]
    length = length_ref[0]
    for n0 in range(0, nstate, SUB):
        for s in range(SUB):
            cols = pl.ds(s * LANES, LANES)
            rows = pl.ds(n0 * SUB + s, SUB, stride=SUB)
            r_ref[rows, :] = -jnp.exp(a_ref[n0:n0 + SUB, cols]) * LOG2E

    def spread(k, carry):
        t0 = pl.multiple_of(k * 16, 16)
        live = (lax.broadcasted_iota(jnp.int32, (16, LANES), 0) + t0 < length).astype(jnp.float32)
        for s in range(SUB):
            cols = pl.ds(s * LANES, LANES)
            v = dt_ref[pl.ds(t0, 16), cols].astype(jnp.float32) + bias_ref[:, cols]
            delta = (jnp.maximum(v, 0.0) + jnp.log1p(jnp.exp(-jnp.abs(v)))) * live
            x = delta * u_ref[pl.ds(t0, 16), cols].astype(jnp.float32)
            for half in range(2):
                rows = pl.ds((t0 + half * SUB) * SUB + s, SUB, stride=SUB)
                d_ref[rows, :] = delta[half * SUB:(half + 1) * SUB]
                x_ref[rows, :] = x[half * SUB:(half + 1) * SUB]
        return carry

    lax.fori_loop(0, tokens // 16, spread, 0)


def prepare(u_rows, dt_rows, a_log, dt_bias, length):
    tokens, width = u_rows.shape
    nstate = a_log.shape[0]
    part = lambda rows: pl.BlockSpec((rows, CHANNELS), lambda i, *_: (0, i))
    tiles = lambda rows: pl.BlockSpec((rows * SUB, LANES), lambda i, *_: (i, 0))
    blocks = width // CHANNELS
    shape = lambda rows: jax.ShapeDtypeStruct((blocks * rows * SUB, LANES), jnp.float32)
    return pl.pallas_call(
        prepare_kernel,
        grid_spec=pltpu.PrefetchScalarGridSpec(
            num_scalar_prefetch=1,
            grid=(blocks,),
            in_specs=[part(tokens), part(tokens), part(nstate), part(1)],
            out_specs=[tiles(tokens), tiles(tokens), tiles(nstate)],
        ),
        out_shape=[shape(tokens), shape(tokens), shape(nstate)],
        compiler_params=pltpu.CompilerParams(vmem_limit_bytes=24 * 2**20),
        cost_estimate=pl.CostEstimate(
            flops=2000 * tokens * width, bytes_accessed=12 * tokens * width, transcendentals=2 * tokens * width),
        name="prepare",
    )(length, u_rows, dt_rows, a_log, dt_bias[None])


def scan_kernel(length_ref, h0_ref, u_ref, d_scr, x_scr, r_scr, b_ref, c_ref, skip_ref, out_ref, last_ref,
                y_scr, h_scr):
    tokens = u_ref.shape[0]
    nstate = h0_ref.shape[0]
    length = length_ref[0]
    for s in range(SUB):
        first = h0_ref[:, s * LANES:(s + 1) * LANES].astype(jnp.float32)
        for n0 in range(0, nstate, SUB):
            h_scr[pl.ds(n0 * SUB + s, SUB, stride=SUB), :] = first[n0:n0 + SUB]

    def advance(t, h):
        row = pl.ds(pl.multiple_of(t * SUB, SUB), SUB)
        d = d_scr[row, :]
        x = x_scr[row, :]
        new = []
        sums = [None, None]
        for n in range(nstate):
            b = b_ref[pl.ds(t * nstate + n, 1), :]
            c = c_ref[pl.ds(t * nstate + n, 1), :]
            g = jnp.exp2(d * r_scr[n * SUB:(n + 1) * SUB, :]) * h[n] + x * b
            new.append(g)
            term = g * c
            sums[n % 2] = term if sums[n % 2] is None else sums[n % 2] + term
        y_scr[row, :] = sums[0] + sums[1]
        return tuple(new)

    h = lax.fori_loop(0, tokens, advance, tuple(h_scr[n * SUB:(n + 1) * SUB, :] for n in range(nstate)), unroll=2)
    for n in range(nstate):
        h_scr[n * SUB:(n + 1) * SUB, :] = h[n]
    for n0 in range(0, nstate, SUB):
        for s in range(SUB):
            last_ref[n0:n0 + SUB, s * LANES:(s + 1) * LANES] = h_scr[pl.ds(n0 * SUB + s, SUB, stride=SUB), :]

    def gather(k, carry):
        t0 = pl.multiple_of(k * 16, 16)
        live = lax.broadcasted_iota(jnp.int32, (16, LANES), 0) + t0 < length
        for s in range(SUB):
            cols = pl.ds(s * LANES, LANES)
            y = jnp.concatenate(
                [y_scr[pl.ds((t0 + half * SUB) * SUB + s, SUB, stride=SUB), :] for half in range(2)], axis=0)
            y = y + skip_ref[:, cols] * u_ref[pl.ds(t0, 16), cols].astype(jnp.float32)
            out_ref[pl.ds(t0, 16), cols] = jnp.where(live, y, 0.0).astype(jnp.bfloat16)
        return carry

    lax.fori_loop(0, tokens // 16, gather, 0)


def splats(bc_rows):
    half, tokens = bc_rows.shape[0] // 2, bc_rows.shape[1]
    return [
        jnp.broadcast_to(jnp.transpose(rows).reshape(-1, 1), (tokens * half, LANES))
        for rows in (bc_rows[:half], bc_rows[half:])
    ]


def selective_scan(start_state, u_rows, prepared, splat, d_skip, length):
    tokens, width = u_rows.shape
    nstate = start_state.shape[0]
    part = lambda rows: pl.BlockSpec((rows, CHANNELS), lambda i, *_: (0, i))
    tiles = lambda rows: pl.BlockSpec((rows * SUB, LANES), lambda i, *_: (i, 0))
    whole = pl.BlockSpec((tokens * nstate, LANES), lambda i, *_: (0, 0))
    work = tokens * nstate * width
    return pl.pallas_call(
        scan_kernel,
        grid_spec=pltpu.PrefetchScalarGridSpec(
            num_scalar_prefetch=1,
            grid=(width // CHANNELS,),
            in_specs=[part(nstate), part(tokens), tiles(tokens), tiles(tokens), tiles(nstate), whole, whole, part(1)],
            out_specs=[part(tokens), part(nstate)],
            scratch_shapes=[
                pltpu.VMEM((tokens * SUB, LANES), jnp.float32),
                pltpu.VMEM((nstate * SUB, LANES), jnp.float32),
            ],
        ),
        out_shape=[
            jax.ShapeDtypeStruct((tokens, width), jnp.bfloat16),
            jax.ShapeDtypeStruct((nstate, width), jnp.float32),
        ],
        cost_estimate=pl.CostEstimate(flops=7 * work, bytes_accessed=14 * tokens * width, transcendentals=work),
        name="selective_scan",
    )(length, start_state, u_rows, *prepared, *splat, d_skip[None])


def attend_kernel(from_ref, order_ref, length_ref, keep_ref, got_ref, sk_ref, sv_ref, q_ref, out_ref,
                  k_scr, v_scr, sems, *, page):
    tokens = q_ref.shape[0]
    pages = order_ref.shape[0]
    prefix = pages * page
    head = pl.program_id(0)
    group = q_ref.shape[1] // HD

    def copies(src_ref, first):
        made = []
        for k in range(pages):
            row = first + order_ref[k] * page
            dst = pl.ds(k * page, page)
            for i, scr in enumerate((k_scr, v_scr)):
                src = pl.ds(pl.multiple_of(row + i * prefix, 16), page)
                made.append(pltpu.make_async_copy(src_ref.at[src], scr.at[dst], sems.at[2 * k + i]))
        tail = pl.ds(prefix, tokens)
        made.append(pltpu.make_async_copy(sk_ref, k_scr.at[tail], sems.at[2 * pages]))
        made.append(pltpu.make_async_copy(sv_ref, v_scr.at[tail], sems.at[2 * pages + 1]))
        for c in made:
            c.start()
        for c in made:
            c.wait()

    @pl.when((head == 0) & (from_ref[0] != 0))
    def _():
        copies(keep_ref, from_ref[1])

    @pl.when((head == 0) & (from_ref[0] == 0))
    def _():
        copies(got_ref, 0)

    cols = pl.ds(pl.multiple_of(head * HD, HD), HD)
    keys = k_scr[:, cols]
    values = v_scr[:, cols]
    t = lax.broadcasted_iota(jnp.int32, (tokens, tokens), 0)
    p = lax.broadcasted_iota(jnp.int32, (tokens, tokens), 1)
    early = jnp.concatenate([p > t] * 2, axis=0)
    late = jnp.concatenate([p <= t] * 2, axis=0)
    live = lax.broadcasted_iota(jnp.int32, (tokens, HD), 0) < length_ref[0]
    scale = 1.0 / math.sqrt(HD)
    for j in range(0, group, 2):
        q = jnp.concatenate([q_ref[:, (j + i) * HD:(j + i + 1) * HD] for i in range(2)], axis=0)
        scores = lax.dot_general(q, keys, (((1,), (1,)), ((), ())), preferred_element_type=jnp.float32) * scale
        scores = jnp.concatenate(
            [
                jnp.where(early, scores[:, :tokens], -1e30),
                scores[:, tokens:prefix],
                jnp.where(late, scores[:, prefix:], -1e30),
            ],
            axis=1,
        )
        e = jnp.exp(scores - jnp.max(scores, axis=1, keepdims=True))
        weights = (e * (1.0 / jnp.sum(e, axis=1, keepdims=True))).astype(jnp.bfloat16)
        mixed = jnp.dot(weights, values, preferred_element_type=jnp.float32)
        for i in range(2):
            out_ref[:, (j + i) * HD:(j + i + 1) * HD] = jnp.where(
                live, mixed[i * tokens:(i + 1) * tokens], 0.0).astype(jnp.bfloat16)


def attend(queries, keep, got, order, origin, suffix_keys, suffix_values, length, page):
    tokens, width = queries.shape
    pages = order.shape[0]
    kv_width = suffix_keys.shape[1]
    rows = pages * page + tokens
    anywhere = pl.BlockSpec(memory_space=pl.ANY)
    heads = pl.BlockSpec((tokens, width // KH), lambda i, *_: (0, i))
    return pl.pallas_call(
        functools.partial(attend_kernel, page=page),
        grid_spec=pltpu.PrefetchScalarGridSpec(
            num_scalar_prefetch=3,
            grid=(KH,),
            in_specs=[anywhere] * 4 + [heads],
            out_specs=heads,
            scratch_shapes=[
                pltpu.VMEM((rows, kv_width), jnp.bfloat16),
                pltpu.VMEM((rows, kv_width), jnp.bfloat16),
                pltpu.SemaphoreType.DMA((2 * pages + 2,)),
            ],
        ),
        out_shape=jax.ShapeDtypeStruct((tokens, width), jnp.bfloat16),
        cost_estimate=pl.CostEstimate(
            flops=4 * tokens * width * rows, bytes_accessed=4 * tokens * width, transcendentals=tokens * QH * rows),
        name="attend",
    )(origin, order, length, keep, got, suffix_keys, suffix_values, queries)


def fill_kernel(side_ref, mine_ref, theirs_ref, store_ref, sems):
    pieces = CHUNKS * STREAMS
    side = side_ref[0]
    made = []
    for i, (src, first) in enumerate(((mine_ref, side * pieces), (theirs_ref, (1 - side) * pieces))):
        for k in range(pieces):
            made.append(pltpu.make_async_copy(src.at[k], store_ref.at[first + k], sems.at[i * pieces + k]))
    for c in made:
        c.start()
    for c in made:
        c.wait()


def new_store(side, mine, theirs, count):
    return pl.pallas_call(
        fill_kernel,
        grid_spec=pltpu.PrefetchScalarGridSpec(
            num_scalar_prefetch=1,
            grid=(1,),
            in_specs=[pl.BlockSpec(mine.shape, lambda i, *_: (0, 0, 0))] * 2,
            out_specs=pl.BlockSpec(memory_space=pl.ANY),
            scratch_shapes=[pltpu.SemaphoreType.DMA((2 * CHUNKS * STREAMS,))],
        ),
        out_shape=jax.ShapeDtypeStruct((count,) + mine.shape[1:], jnp.bfloat16),
        name="new_store",
    )(side, mine, theirs)


def plan_kernel(where_ref, ahead_ref, rank_ref, start_ref, gives_ref, takes_ref, steps_ref, waiting, sent, sends):
    ring, lanes = ahead_ref.shape
    slots = lanes // 2
    lane = lax.broadcasted_iota(jnp.int32, (ring, lanes), 1)
    low = lane < slots
    name = jnp.where(low, lane, lane - slots) * CHUNKS + 1
    ours = (lax.broadcasted_iota(jnp.int32, (1, lanes), 1) < slots) == (where_ref[2] == 0)
    waiting[...] = start_ref[...]
    sent[...] = jnp.zeros_like(sent)
    gives_ref[pl.ds(0, 2 * SUB), :] = jnp.zeros((2 * SUB, lanes), jnp.int32)
    takes_ref[pl.ds(0, 2 * SUB), :] = jnp.zeros((2 * SUB, lanes), jnp.int32)

    def step(carry):
        t, _ = carry
        now = waiting[...]
        done = sent[...]
        urgent = jnp.where(now > 0, rank_ref[...], 0)
        best = jnp.where(
            low,
            jnp.max(jnp.where(low, urgent, 0), axis=1, keepdims=True),
            jnp.max(jnp.where(low, 0, urgent), axis=1, keepdims=True),
        )
        chosen = jnp.where((urgent == best) & (now > 0), 1, 0)
        sends[...] = jnp.where(chosen > 0, name + done, 0)
        arrived = jnp.concatenate([chosen[ring - 1:], chosen[:ring - 1]], axis=0)
        left = now - chosen + jnp.where(ahead_ref[...] > 0, arrived, 0)
        waiting[...] = left
        sent[...] = done + chosen
        row = lambda k: jnp.where(ours, sends[pl.ds(where_ref[k], 1), :], 0)
        gives_ref[pl.ds(t, 1), :] = row(0)
        takes_ref[pl.ds(t + 1, 1), :] = row(1)
        return t + 1, jnp.max(left) > 0

    steps = lax.while_loop(lambda carry: carry[1], step, (jnp.int32(0), jnp.max(start_ref[...]) > 0))[0]
    gives_ref[pl.ds(steps, 1), :] = jnp.zeros((1, lanes), jnp.int32)
    steps_ref[0] = steps


def plan(source, chip, side, ring, slots):
    slot = jnp.arange(slots, dtype=jnp.int32)
    home = slot // 2
    place = jnp.arange(ring, dtype=jnp.int32)
    reader = jnp.arange(source.shape[0], dtype=jnp.int32) // 2
    away = jnp.mod(reader[:, None] - home[None, :], ring)
    wanted = source[:, None] == slot[None, :]
    near = away <= ring // 2
    reach = jnp.concatenate([
        jnp.max(jnp.where(wanted & near, away, 0), axis=0),
        jnp.max(jnp.where(wanted & ~near, ring - away, 0), axis=0),
    ])
    gone = jnp.concatenate([
        jnp.mod(place[:, None] - home[None, :], ring),
        jnp.mod(place[:, None] + home[None, :], ring),
    ], axis=1)
    ahead = jnp.maximum(reach[None, :] - gone, 0)
    start = jnp.where((gone == 0) & (ahead > 0), CHUNKS, 0)
    rank = ahead * slots + jnp.concatenate([slot, slot])[None, :]
    most = slots * CHUNKS * (ring // 2)
    seat = jnp.where(side == 0, chip, jnp.mod(-chip, ring))
    where = jnp.stack([seat, jnp.mod(seat - 1, ring), side])
    gives, takes, steps = pl.pallas_call(
        plan_kernel,
        grid_spec=pltpu.PrefetchScalarGridSpec(
            num_scalar_prefetch=1,
            grid=(1,),
            in_specs=[pl.BlockSpec((ring, 2 * slots), lambda i, *_: (0, 0))] * 3,
            out_specs=[
                pl.BlockSpec((most + 2 * SUB, 2 * slots), lambda i, *_: (0, 0)),
                pl.BlockSpec((most + 2 * SUB, 2 * slots), lambda i, *_: (0, 0)),
                pl.BlockSpec(memory_space=pltpu.SMEM),
            ],
            scratch_shapes=[pltpu.VMEM((ring, 2 * slots), jnp.int32)] * 3,
        ),
        out_shape=[
            jax.ShapeDtypeStruct((most + 2 * SUB, 2 * slots), jnp.int32),
            jax.ShapeDtypeStruct((most + 2 * SUB, 2 * slots), jnp.int32),
            jax.ShapeDtypeStruct((1,), jnp.int32),
        ],
        name="plan",
    )(where, ahead, rank, start)
    return gives, takes, steps[0]


def turn_kernel(gives_ref, takes_ref, at_ref, store_in, arrived, store, out, sems, *, line, stream, ring):
    del store_in
    chip, side = at_ref[0], at_ref[1]

    def piece(name, otherwise):
        slot = name // CHUNKS
        home = slot // 2
        behind = jnp.where(side == 0, chip - home, home - chip)
        behind = jnp.where(behind < 0, behind + ring, behind)
        index = ((behind * 2 + slot % 2) * CHUNKS + name % CHUNKS) * STREAMS + stream
        return jnp.where(name < 0, otherwise, index)

    give = piece(jnp.max(gives_ref[line:line + 1, :]) - 1, stream)
    take = piece(jnp.max(takes_ref[line:line + 1, :]) - 1, store.shape[0] - 1)
    keep = pltpu.make_async_copy(arrived, store.at[take], sems.at[0])
    direct = pltpu.make_async_copy(arrived, out, sems.at[1])
    stored = pltpu.make_async_copy(store.at[give], out, sems.at[1])
    keep.start()

    @pl.when(give == take)
    def _():
        direct.start()

    @pl.when(give != take)
    def _():
        stored.start()

    keep.wait()
    direct.wait()


def turn(gives, takes, at, store, arrived, line, stream, ring):
    vmem = pl.BlockSpec(memory_space=pltpu.VMEM)
    anywhere = pl.BlockSpec(memory_space=pl.ANY)
    return pl.pallas_call(
        functools.partial(turn_kernel, line=line, stream=stream, ring=ring),
        in_specs=[vmem, vmem, pl.BlockSpec(memory_space=pltpu.SMEM), anywhere, vmem],
        out_specs=[anywhere, vmem],
        out_shape=[jax.ShapeDtypeStruct(store.shape, store.dtype), jax.ShapeDtypeStruct(arrived.shape, arrived.dtype)],
        scratch_shapes=[pltpu.SemaphoreType.DMA((2,))],
        input_output_aliases={3: 0},
        compiler_params=pltpu.CompilerParams(vmem_limit_bytes=8 * 2**20),
        name="turn",
    )(gives, takes, at, store, arrived)


def relay(store, gives, takes, steps, at, ring, beside):
    count = 2 * ring
    onward = [(i, (i + 2 - 4 * (i % 2)) % count) for i in range(count)]
    lines = lambda table, t: lax.dynamic_slice_in_dim(table, t, SUB, 0)

    def some(depth, beside=lambda: ((), ())):
        def body(carry):
            t, store, held, give, take = carry
            held = list(held)
            early, late = beside()
            after = None
            for line in range(depth):
                for stream in range(STREAMS):
                    store, out = turn(give, take, at, store, held[stream], line, stream, ring)
                    held[stream] = lax.ppermute(out, "req", onward)
                if line == 0:
                    after = lines(gives, t + depth), lines(takes, t + depth)
                    store, early, after = lax.optimization_barrier((store, early, after))
            held, after, late = lax.optimization_barrier((tuple(held), after, late))
            return (t + depth, store, held, *after), early, late

        return body

    blank = jnp.zeros(store.shape[1:], store.dtype)
    carry = (jnp.int32(0), store, (blank,) * STREAMS, lines(gives, 0), lines(takes, 0))
    carry, early, late = some(FIRST, beside)(carry)
    carry = lax.while_loop(lambda c: c[0] + DEPTH <= steps, lambda c: some(DEPTH)(c)[0], carry)
    carry = lax.while_loop(lambda c: c[0] < steps, lambda c: some(1)(c)[0], carry)
    _, store, held, give, take = carry
    for stream in range(STREAMS):
        store = turn(give, take, at, store, held[stream], 0, stream, ring)[0]
    return store, early, late


def local(
    cache_states,
    pool_keys,
    pool_values,
    slot_prefix,
    page_table,
    prefix_id,
    lengths,
    queries,
    suffix_keys,
    suffix_values,
    u_in,
    dt_raw,
    bc_in,
    a_log,
    dt_bias,
    d_skip,
):
    me = lax.axis_index("req")
    side = jnp.mod(me, 2)
    chip = me // 2
    slots = slot_prefix.shape[0]
    ring = slots // 2
    swap = [(i, i ^ 1) for i in range(slots)]
    matches = (slot_prefix[None, :] == prefix_id[:, None]).astype(jnp.int32)
    source = jnp.sum(matches * jnp.arange(slots, dtype=jnp.int32)[None, :], axis=1)

    pages, page, kv_width = pool_keys.shape
    nstate, width = a_log.shape
    pieces = CHUNKS * STREAMS
    state_rows = nstate * width // kv_width
    state = cache_states[0].reshape(nstate, width // kv_width, kv_width).transpose(1, 0, 2)
    mine = jnp.concatenate([
        state.reshape(state_rows, kv_width),
        pool_keys.reshape(pages * page, kv_width),
        pool_values.reshape(pages * page, kv_width),
    ], axis=0)
    rows = mine.shape[0]
    mine = mine.reshape(pieces, rows // pieces, kv_width)
    theirs = lax.ppermute(mine, "req", swap)
    at = jnp.stack([chip, side])
    gives, takes, steps = plan(source, chip, side, ring, slots)
    store = new_store(side[None], mine, theirs, (ring // 2 + 1) * 2 * pieces + 1)

    def find(request):
        slot = source[request]
        ahead = jnp.mod(chip - slot // 2, ring)
        behind = jnp.where(side == 0, ahead, jnp.mod(-ahead, ring))
        here = jnp.where(side == 0, ahead <= ring // 2, (ahead > ring // 2) | (ahead == 0))
        return here, jnp.where(here, behind * 2 + jnp.mod(slot, 2), 0) * rows

    def beside():
        early = splats(bc_in[0]), page_table[prefix_id[me]], find(me), find(me + 1 - 2 * side)[1]
        return early, prepare(u_in, dt_raw, a_log, dt_bias, lengths)

    store, early, prepared = relay(store, gives, takes, steps, at, ring, beside)
    splat, order, (here, first), other = early
    flat = store.reshape(-1, kv_width)
    got_state = lax.ppermute(lax.dynamic_slice_in_dim(flat, other, state_rows, 0), "req", swap)
    got = lax.ppermute(lax.dynamic_slice_in_dim(flat, other + state_rows, rows - state_rows, 0), "req", swap)
    start_state = jnp.where(here, lax.dynamic_slice_in_dim(flat, first, state_rows, 0), got_state)
    start_state = start_state.reshape(width // kv_width, nstate, kv_width).transpose(1, 0, 2).reshape(nstate, width)
    mamba_out, last_state = selective_scan(start_state, u_in, prepared, splat, d_skip, lengths)
    origin = jnp.stack([here.astype(jnp.int32), first + state_rows])
    attn_out = attend(queries, flat, got, order, origin, suffix_keys, suffix_values, lengths, page)
    return (mamba_out, attn_out, last_state[None])


def solution(mesh):
    placed = (
        P(("groups", "req"), None, None),
        P(("groups", "req"), None, None),
        P(("groups", "req"), None, None),
        P("groups"),
        P("groups", None),
        P("groups"),
        P(("groups", "req")),
        P(("groups", "req"), None),
        P(("groups", "req"), None),
        P(("groups", "req"), None),
        P(("groups", "req"), None),
        P(("groups", "req"), None),
        P(("groups", "req"), None, None),
        P(),
        P(),
        P(),
    )
    return jax.shard_map(
        local,
        mesh=mesh,
        in_specs=placed,
        out_specs=(
            P(("groups", "req"), None),
            P(("groups", "req"), None),
            P(("groups", "req"), None, None),
        ),
        check_vma=False,
    )
```

```python
import functools
import math

import jax
import jax.numpy as jnp
from jax import lax
from jax.experimental import pallas as pl
from jax.experimental.pallas import tpu as pltpu
from jax.sharding import PartitionSpec as P

QH = 32
KH = 4
HD = 128

LANES = 128
SUB = 8
CHUNKS = 2
STREAMS = 2
FIRST = 20
LINES = 32
DEPTH = 2
CHANNELS = SUB * LANES
LOG2E = math.log2(math.e)


def prepare_kernel(length_ref, u_ref, dt_ref, a_ref, bias_ref, d_ref, x_ref, r_ref):
    tokens = u_ref.shape[0]
    nstate = a_ref.shape[0]
    length = length_ref[0]
    for n0 in range(0, nstate, SUB):
        for s in range(SUB):
            cols = pl.ds(s * LANES, LANES)
            rows = pl.ds(n0 * SUB + s, SUB, stride=SUB)
            r_ref[rows, :] = -jnp.exp(a_ref[n0:n0 + SUB, cols]) * LOG2E

    def spread(k, carry):
        t0 = pl.multiple_of(k * 16, 16)
        live = (lax.broadcasted_iota(jnp.int32, (16, LANES), 0) + t0 < length).astype(jnp.float32)
        for s in range(SUB):
            cols = pl.ds(s * LANES, LANES)
            v = dt_ref[pl.ds(t0, 16), cols].astype(jnp.float32) + bias_ref[:, cols]
            delta = (jnp.maximum(v, 0.0) + jnp.log1p(jnp.exp(-jnp.abs(v)))) * live
            x = delta * u_ref[pl.ds(t0, 16), cols].astype(jnp.float32)
            for half in range(2):
                rows = pl.ds((t0 + half * SUB) * SUB + s, SUB, stride=SUB)
                d_ref[rows, :] = delta[half * SUB:(half + 1) * SUB]
                x_ref[rows, :] = x[half * SUB:(half + 1) * SUB]
        return carry

    lax.fori_loop(0, tokens // 16, spread, 0)


def prepare(u_rows, dt_rows, a_log, dt_bias, length):
    tokens, width = u_rows.shape
    nstate = a_log.shape[0]
    part = lambda rows: pl.BlockSpec((rows, CHANNELS), lambda i, *_: (0, i))
    tiles = lambda rows: pl.BlockSpec((rows * SUB, LANES), lambda i, *_: (i, 0))
    blocks = width // CHANNELS
    shape = lambda rows: jax.ShapeDtypeStruct((blocks * rows * SUB, LANES), jnp.float32)
    return pl.pallas_call(
        prepare_kernel,
        grid_spec=pltpu.PrefetchScalarGridSpec(
            num_scalar_prefetch=1,
            grid=(blocks,),
            in_specs=[part(tokens), part(tokens), part(nstate), part(1)],
            out_specs=[tiles(tokens), tiles(tokens), tiles(nstate)],
        ),
        out_shape=[shape(tokens), shape(tokens), shape(nstate)],
        cost_estimate=pl.CostEstimate(
            flops=2000 * tokens * width, bytes_accessed=12 * tokens * width, transcendentals=2 * tokens * width),
        name="prepare",
    )(length, u_rows, dt_rows, a_log, dt_bias[None])


def scan_kernel(length_ref, h0_ref, u_ref, d_scr, x_scr, r_scr, b_ref, c_ref, skip_ref, out_ref, last_ref,
                y_scr, h_scr):
    tokens = u_ref.shape[0]
    nstate = h0_ref.shape[0]
    length = length_ref[0]
    for s in range(SUB):
        first = h0_ref[:, s * LANES:(s + 1) * LANES].astype(jnp.float32)
        for n0 in range(0, nstate, SUB):
            h_scr[pl.ds(n0 * SUB + s, SUB, stride=SUB), :] = first[n0:n0 + SUB]

    def advance(t, h):
        row = pl.ds(pl.multiple_of(t * SUB, SUB), SUB)
        d = d_scr[row, :]
        x = x_scr[row, :]
        new = []
        sums = [None, None]
        for n in range(nstate):
            b = b_ref[pl.ds(t * nstate + n, 1), :]
            c = c_ref[pl.ds(t * nstate + n, 1), :]
            g = jnp.exp2(d * r_scr[n * SUB:(n + 1) * SUB, :]) * h[n] + x * b
            new.append(g)
            term = g * c
            sums[n % 2] = term if sums[n % 2] is None else sums[n % 2] + term
        y_scr[row, :] = sums[0] + sums[1]
        return tuple(new)

    h = lax.fori_loop(0, tokens, advance, tuple(h_scr[n * SUB:(n + 1) * SUB, :] for n in range(nstate)), unroll=4)
    for n in range(nstate):
        h_scr[n * SUB:(n + 1) * SUB, :] = h[n]
    for n0 in range(0, nstate, SUB):
        for s in range(SUB):
            last_ref[n0:n0 + SUB, s * LANES:(s + 1) * LANES] = h_scr[pl.ds(n0 * SUB + s, SUB, stride=SUB), :]

    def gather(k, carry):
        t0 = pl.multiple_of(k * 16, 16)
        live = lax.broadcasted_iota(jnp.int32, (16, LANES), 0) + t0 < length
        for s in range(SUB):
            cols = pl.ds(s * LANES, LANES)
            y = jnp.concatenate(
                [y_scr[pl.ds((t0 + half * SUB) * SUB + s, SUB, stride=SUB), :] for half in range(2)], axis=0)
            y = y + skip_ref[:, cols] * u_ref[pl.ds(t0, 16), cols].astype(jnp.float32)
            out_ref[pl.ds(t0, 16), cols] = jnp.where(live, y, 0.0).astype(jnp.bfloat16)
        return carry

    lax.fori_loop(0, tokens // 16, gather, 0)


def splats(bc_rows):
    half, tokens = bc_rows.shape[0] // 2, bc_rows.shape[1]
    return [
        jnp.broadcast_to(jnp.transpose(rows).reshape(-1, 1), (tokens * half, LANES))
        for rows in (bc_rows[:half], bc_rows[half:])
    ]


def selective_scan(start_state, u_rows, prepared, splat, d_skip, length):
    tokens, width = u_rows.shape
    nstate = start_state.shape[0]
    part = lambda rows: pl.BlockSpec((rows, CHANNELS), lambda i, *_: (0, i))
    tiles = lambda rows: pl.BlockSpec((rows * SUB, LANES), lambda i, *_: (i, 0))
    whole = pl.BlockSpec((tokens * nstate, LANES), lambda i, *_: (0, 0))
    work = tokens * nstate * width
    return pl.pallas_call(
        scan_kernel,
        grid_spec=pltpu.PrefetchScalarGridSpec(
            num_scalar_prefetch=1,
            grid=(width // CHANNELS,),
            in_specs=[part(nstate), part(tokens), tiles(tokens), tiles(tokens), tiles(nstate), whole, whole, part(1)],
            out_specs=[part(tokens), part(nstate)],
            scratch_shapes=[
                pltpu.VMEM((tokens * SUB, LANES), jnp.float32),
                pltpu.VMEM((nstate * SUB, LANES), jnp.float32),
            ],
        ),
        out_shape=[
            jax.ShapeDtypeStruct((tokens, width), jnp.bfloat16),
            jax.ShapeDtypeStruct((nstate, width), jnp.float32),
        ],
        cost_estimate=pl.CostEstimate(flops=7 * work, bytes_accessed=14 * tokens * width, transcendentals=work),
        name="selective_scan",
    )(length, start_state, u_rows, *prepared, *splat, d_skip[None])


def attend_kernel(from_ref, order_ref, length_ref, keep_ref, got_ref, sk_ref, sv_ref, q_ref, out_ref,
                  k_scr, v_scr, sems, *, page):
    tokens = q_ref.shape[0]
    pages = order_ref.shape[0]
    prefix = pages * page
    head = pl.program_id(0)
    group = q_ref.shape[1] // HD

    def copies(src_ref, first):
        made = []
        for k in range(pages):
            row = first + order_ref[k] * page
            dst = pl.ds(k * page, page)
            for i, scr in enumerate((k_scr, v_scr)):
                src = pl.ds(pl.multiple_of(row + i * prefix, 16), page)
                made.append(pltpu.make_async_copy(src_ref.at[src], scr.at[dst], sems.at[2 * k + i]))
        tail = pl.ds(prefix, tokens)
        made.append(pltpu.make_async_copy(sk_ref, k_scr.at[tail], sems.at[2 * pages]))
        made.append(pltpu.make_async_copy(sv_ref, v_scr.at[tail], sems.at[2 * pages + 1]))
        for c in made:
            c.start()
        for c in made:
            c.wait()

    @pl.when((head == 0) & (from_ref[0] != 0))
    def _():
        copies(keep_ref, from_ref[1])

    @pl.when((head == 0) & (from_ref[0] == 0))
    def _():
        copies(got_ref, 0)

    cols = pl.ds(pl.multiple_of(head * HD, HD), HD)
    keys = k_scr[:, cols]
    values = v_scr[:, cols]
    t = lax.broadcasted_iota(jnp.int32, (tokens, tokens), 0)
    p = lax.broadcasted_iota(jnp.int32, (tokens, tokens), 1)
    early = jnp.concatenate([p > t] * 2, axis=0)
    late = jnp.concatenate([p <= t] * 2, axis=0)
    live = lax.broadcasted_iota(jnp.int32, (tokens, HD), 0) < length_ref[0]
    scale = 1.0 / math.sqrt(HD)
    for j in range(0, group, 2):
        q = jnp.concatenate([q_ref[:, (j + i) * HD:(j + i + 1) * HD] for i in range(2)], axis=0)
        scores = lax.dot_general(q, keys, (((1,), (1,)), ((), ())), preferred_element_type=jnp.float32) * scale
        scores = jnp.concatenate(
            [
                jnp.where(early, scores[:, :tokens], -1e30),
                scores[:, tokens:prefix],
                jnp.where(late, scores[:, prefix:], -1e30),
            ],
            axis=1,
        )
        e = jnp.exp(scores - jnp.max(scores, axis=1, keepdims=True))
        weights = (e * (1.0 / jnp.sum(e, axis=1, keepdims=True))).astype(jnp.bfloat16)
        mixed = jnp.dot(weights, values, preferred_element_type=jnp.float32)
        for i in range(2):
            out_ref[:, (j + i) * HD:(j + i + 1) * HD] = jnp.where(
                live, mixed[i * tokens:(i + 1) * tokens], 0.0).astype(jnp.bfloat16)


def attend(queries, keep, got, order, origin, suffix_keys, suffix_values, length, page):
    tokens, width = queries.shape
    pages = order.shape[0]
    kv_width = suffix_keys.shape[1]
    rows = pages * page + tokens
    anywhere = pl.BlockSpec(memory_space=pl.ANY)
    heads = pl.BlockSpec((tokens, width // KH), lambda i, *_: (0, i))
    return pl.pallas_call(
        functools.partial(attend_kernel, page=page),
        grid_spec=pltpu.PrefetchScalarGridSpec(
            num_scalar_prefetch=3,
            grid=(KH,),
            in_specs=[anywhere] * 4 + [heads],
            out_specs=heads,
            scratch_shapes=[
                pltpu.VMEM((rows, kv_width), jnp.bfloat16),
                pltpu.VMEM((rows, kv_width), jnp.bfloat16),
                pltpu.SemaphoreType.DMA((2 * pages + 2,)),
            ],
        ),
        out_shape=jax.ShapeDtypeStruct((tokens, width), jnp.bfloat16),
        cost_estimate=pl.CostEstimate(
            flops=4 * tokens * width * rows, bytes_accessed=4 * tokens * width, transcendentals=tokens * QH * rows),
        name="attend",
    )(origin, order, length, keep, got, suffix_keys, suffix_values, queries)


def fill_kernel(side_ref, mine_ref, theirs_ref, store_ref, sems):
    pieces = CHUNKS * STREAMS
    side = side_ref[0]
    made = []
    for i, (src, first) in enumerate(((mine_ref, side * pieces), (theirs_ref, (1 - side) * pieces))):
        for k in range(pieces):
            made.append(pltpu.make_async_copy(src.at[k], store_ref.at[first + k], sems.at[i * pieces + k]))
    for c in made:
        c.start()
    for c in made:
        c.wait()


def new_store(side, mine, theirs, count):
    return pl.pallas_call(
        fill_kernel,
        grid_spec=pltpu.PrefetchScalarGridSpec(
            num_scalar_prefetch=1,
            grid=(1,),
            in_specs=[pl.BlockSpec(mine.shape, lambda i, *_: (0, 0, 0))] * 2,
            out_specs=pl.BlockSpec(memory_space=pl.ANY),
            scratch_shapes=[pltpu.SemaphoreType.DMA((2 * CHUNKS * STREAMS,))],
        ),
        out_shape=jax.ShapeDtypeStruct((count,) + mine.shape[1:], jnp.bfloat16),
        name="new_store",
    )(side, mine, theirs)


def plan_kernel(where_ref, ahead_ref, rank_ref, start_ref, gives_ref, takes_ref, steps_ref, waiting, sent, sends):
    ring, lanes = ahead_ref.shape
    slots = lanes // 2
    lane = lax.broadcasted_iota(jnp.int32, (ring, lanes), 1)
    low = lane < slots
    name = jnp.where(low, lane, lane - slots) * CHUNKS + 1
    ours = (lax.broadcasted_iota(jnp.int32, (1, lanes), 1) < slots) == (where_ref[2] == 0)
    waiting[...] = start_ref[...]
    sent[...] = jnp.zeros_like(sent)
    gives_ref[pl.ds(0, LINES), :] = jnp.zeros((LINES, lanes), jnp.int32)
    takes_ref[pl.ds(0, LINES), :] = jnp.zeros((LINES, lanes), jnp.int32)

    def step(carry):
        t, _ = carry
        now = waiting[...]
        done = sent[...]
        urgent = jnp.where(now > 0, rank_ref[...], 0)
        best = jnp.where(
            low,
            jnp.max(jnp.where(low, urgent, 0), axis=1, keepdims=True),
            jnp.max(jnp.where(low, 0, urgent), axis=1, keepdims=True),
        )
        chosen = jnp.where((urgent == best) & (now > 0), 1, 0)
        sends[...] = jnp.where(chosen > 0, name + done, 0)
        arrived = jnp.concatenate([chosen[ring - 1:], chosen[:ring - 1]], axis=0)
        left = now - chosen + jnp.where(ahead_ref[...] > 0, arrived, 0)
        waiting[...] = left
        sent[...] = done + chosen
        row = lambda k: jnp.where(ours, sends[pl.ds(where_ref[k], 1), :], 0)
        gives_ref[pl.ds(t, 1), :] = row(0)
        takes_ref[pl.ds(t + 1, 1), :] = row(1)
        return t + 1, jnp.max(left) > 0

    steps = lax.while_loop(lambda carry: carry[1], step, (jnp.int32(0), jnp.max(start_ref[...]) > 0))[0]
    gives_ref[pl.ds(steps, 1), :] = jnp.zeros((1, lanes), jnp.int32)
    steps_ref[0] = steps


def plan(source, chip, side, ring, slots):
    slot = jnp.arange(slots, dtype=jnp.int32)
    home = slot // 2
    place = jnp.arange(ring, dtype=jnp.int32)
    reader = jnp.arange(source.shape[0], dtype=jnp.int32) // 2
    away = jnp.mod(reader[:, None] - home[None, :], ring)
    wanted = source[:, None] == slot[None, :]
    near = away <= ring // 2
    reach = jnp.concatenate([
        jnp.max(jnp.where(wanted & near, away, 0), axis=0),
        jnp.max(jnp.where(wanted & ~near, ring - away, 0), axis=0),
    ])
    gone = jnp.concatenate([
        jnp.mod(place[:, None] - home[None, :], ring),
        jnp.mod(place[:, None] + home[None, :], ring),
    ], axis=1)
    ahead = jnp.maximum(reach[None, :] - gone, 0)
    start = jnp.where((gone == 0) & (ahead > 0), CHUNKS, 0)
    rank = ahead * slots + jnp.concatenate([slot, slot])[None, :]
    most = slots * CHUNKS * (ring // 2)
    seat = jnp.where(side == 0, chip, jnp.mod(-chip, ring))
    where = jnp.stack([seat, jnp.mod(seat - 1, ring), side])
    gives, takes, steps = pl.pallas_call(
        plan_kernel,
        grid_spec=pltpu.PrefetchScalarGridSpec(
            num_scalar_prefetch=1,
            grid=(1,),
            in_specs=[pl.BlockSpec((ring, 2 * slots), lambda i, *_: (0, 0))] * 3,
            out_specs=[
                pl.BlockSpec((most + LINES, 2 * slots), lambda i, *_: (0, 0)),
                pl.BlockSpec((most + LINES, 2 * slots), lambda i, *_: (0, 0)),
                pl.BlockSpec(memory_space=pltpu.SMEM),
            ],
            scratch_shapes=[pltpu.VMEM((ring, 2 * slots), jnp.int32)] * 3,
        ),
        out_shape=[
            jax.ShapeDtypeStruct((most + LINES, 2 * slots), jnp.int32),
            jax.ShapeDtypeStruct((most + LINES, 2 * slots), jnp.int32),
            jax.ShapeDtypeStruct((1,), jnp.int32),
        ],
        name="plan",
    )(where, ahead, rank, start)
    return gives, takes, steps[0]


def piece(name, otherwise, at_ref, stream, ring):
    slot = name // CHUNKS
    home = slot // 2
    behind = jnp.where(at_ref[1] == 0, at_ref[0] - home, home - at_ref[0])
    behind = jnp.where(behind < 0, behind + ring, behind)
    index = ((behind * 2 + slot % 2) * CHUNKS + name % CHUNKS) * STREAMS + stream
    return jnp.where(name < 0, otherwise, index)


def turn_kernel(gives_ref, takes_ref, at_ref, store_in, arrived, store, out, sems, *, line, stream, ring):
    del store_in
    give = piece(jnp.max(gives_ref[line:line + 1, :]) - 1, stream, at_ref, stream, ring)
    take = piece(jnp.max(takes_ref[line:line + 1, :]) - 1, store.shape[0] - 1, at_ref, stream, ring)
    keep = pltpu.make_async_copy(arrived, store.at[take], sems.at[0])
    direct = pltpu.make_async_copy(arrived, out, sems.at[1])
    stored = pltpu.make_async_copy(store.at[give], out, sems.at[1])
    keep.start()

    @pl.when(give == take)
    def _():
        direct.start()

    @pl.when(give != take)
    def _():
        stored.start()

    keep.wait()
    direct.wait()


def settle_kernel(takes_ref, at_ref, store_in, a_ref, b_ref, store, sems, *, ring):
    del store_in
    name = jnp.max(takes_ref[0:1, :]) - 1

    @pl.when(name >= 0)
    def _():
        made = [
            pltpu.make_async_copy(ref, store.at[piece(name, 0, at_ref, stream, ring)], sems.at[stream])
            for stream, ref in enumerate((a_ref, b_ref))
        ]
        for c in made:
            c.start()
        for c in made:
            c.wait()


def settle(takes, at, store, held, ring):
    vmem = pl.BlockSpec(memory_space=pltpu.VMEM)
    anywhere = pl.BlockSpec(memory_space=pl.ANY)
    return pl.pallas_call(
        functools.partial(settle_kernel, ring=ring),
        in_specs=[vmem, pl.BlockSpec(memory_space=pltpu.SMEM), anywhere, vmem, vmem],
        out_specs=anywhere,
        out_shape=jax.ShapeDtypeStruct(store.shape, store.dtype),
        scratch_shapes=[pltpu.SemaphoreType.DMA((STREAMS,))],
        input_output_aliases={2: 0},
        compiler_params=pltpu.CompilerParams(vmem_limit_bytes=8 * 2**20),
        name="settle",
    )(takes, at, store, *held)


def turn(gives, takes, at, store, arrived, line, stream, ring):
    vmem = pl.BlockSpec(memory_space=pltpu.VMEM)
    anywhere = pl.BlockSpec(memory_space=pl.ANY)
    return pl.pallas_call(
        functools.partial(turn_kernel, line=line, stream=stream, ring=ring),
        in_specs=[vmem, vmem, pl.BlockSpec(memory_space=pltpu.SMEM), anywhere, vmem],
        out_specs=[anywhere, vmem],
        out_shape=[jax.ShapeDtypeStruct(store.shape, store.dtype), jax.ShapeDtypeStruct(arrived.shape, arrived.dtype)],
        scratch_shapes=[pltpu.SemaphoreType.DMA((2,))],
        input_output_aliases={3: 0},
        compiler_params=pltpu.CompilerParams(vmem_limit_bytes=8 * 2**20),
        name="turn",
    )(gives, takes, at, store, arrived)


def relay(store, gives, takes, steps, at, ring, beside):
    count = 2 * ring
    onward = [(i, (i + 2 - 4 * (i % 2)) % count) for i in range(count)]
    lines = lambda table, t, rows=SUB: lax.dynamic_slice_in_dim(table, t, rows, 0)

    def some(depth, beside=tuple):
        def body(carry):
            t, store, held, give, take = carry
            held = list(held)
            extra = beside()
            after = None
            for line in range(depth):
                for stream in range(STREAMS):
                    store, out = turn(give, take, at, store, held[stream], line, stream, ring)
                    held[stream] = lax.ppermute(out, "req", onward)
                if line == 0:
                    after = lines(gives, t + depth), lines(takes, t + depth)
                    store, extra, after = lax.optimization_barrier((store, extra, after))
            held, after = lax.optimization_barrier((tuple(held), after))
            return (t + depth, store, held, *after), extra

        return body

    blank = jnp.zeros(store.shape[1:], store.dtype)
    carry = (jnp.int32(0), store, (blank,) * STREAMS, gives[:LINES], takes[:LINES])
    carry, extra = some(FIRST, beside)(carry)
    carry = lax.while_loop(lambda c: c[0] + DEPTH <= steps, lambda c: some(DEPTH)(c)[0], carry)
    carry = lax.while_loop(lambda c: c[0] < steps, lambda c: some(1)(c)[0], carry)
    _, store, held, give, take = carry
    return settle(take, at, store, held, ring), extra


def local(
    cache_states,
    pool_keys,
    pool_values,
    slot_prefix,
    page_table,
    prefix_id,
    lengths,
    queries,
    suffix_keys,
    suffix_values,
    u_in,
    dt_raw,
    bc_in,
    a_log,
    dt_bias,
    d_skip,
):
    me = lax.axis_index("req")
    side = jnp.mod(me, 2)
    chip = me // 2
    slots = slot_prefix.shape[0]
    ring = slots // 2
    swap = [(i, i ^ 1) for i in range(slots)]
    matches = (slot_prefix[None, :] == prefix_id[:, None]).astype(jnp.int32)
    source = jnp.sum(matches * jnp.arange(slots, dtype=jnp.int32)[None, :], axis=1)

    pages, page, kv_width = pool_keys.shape
    nstate, width = a_log.shape
    pieces = CHUNKS * STREAMS
    state_rows = nstate * width // kv_width
    state = cache_states[0].reshape(nstate, width // kv_width, kv_width).transpose(1, 0, 2)
    mine = jnp.concatenate([
        state.reshape(state_rows, kv_width),
        pool_keys.reshape(pages * page, kv_width),
        pool_values.reshape(pages * page, kv_width),
    ], axis=0)
    rows = mine.shape[0]
    mine = mine.reshape(pieces, rows // pieces, kv_width)
    theirs = lax.ppermute(mine, "req", swap)
    at = jnp.stack([chip, side])
    gives, takes, steps = plan(source, chip, side, ring, slots)
    store = new_store(side[None], mine, theirs, (ring // 2 + 1) * 2 * pieces + 1)

    def find(request):
        slot = source[request]
        ahead = jnp.mod(chip - slot // 2, ring)
        behind = jnp.where(side == 0, ahead, jnp.mod(-ahead, ring))
        here = jnp.where(side == 0, ahead <= ring // 2, (ahead > ring // 2) | (ahead == 0))
        return here, jnp.where(here, behind * 2 + jnp.mod(slot, 2), 0) * rows

    def beside():
        return (
            prepare(u_in, dt_raw, a_log, dt_bias, lengths), splats(bc_in[0]), page_table[prefix_id[me]], find(me),
            find(me + 1 - 2 * side)[1])

    store, extra = relay(store, gives, takes, steps, at, ring, beside)
    prepared, splat, order, (here, first), other = extra
    flat = store.reshape(-1, kv_width)
    got_state = lax.ppermute(lax.dynamic_slice_in_dim(flat, other, state_rows, 0), "req", swap)
    got = lax.ppermute(lax.dynamic_slice_in_dim(flat, other + state_rows, rows - state_rows, 0), "req", swap)
    start_state = jnp.where(here, lax.dynamic_slice_in_dim(flat, first, state_rows, 0), got_state)
    start_state = start_state.reshape(width // kv_width, nstate, kv_width).transpose(1, 0, 2).reshape(nstate, width)
    mamba_out, last_state = selective_scan(start_state, u_in, prepared, splat, d_skip, lengths)
    origin = jnp.stack([here.astype(jnp.int32), first + state_rows])
    attn_out = attend(queries, flat, got, order, origin, suffix_keys, suffix_values, lengths, page)
    return (mamba_out, attn_out, last_state[None])


def solution(mesh):
    placed = (
        P(("groups", "req"), None, None),
        P(("groups", "req"), None, None),
        P(("groups", "req"), None, None),
        P("groups"),
        P("groups", None),
        P("groups"),
        P(("groups", "req")),
        P(("groups", "req"), None),
        P(("groups", "req"), None),
        P(("groups", "req"), None),
        P(("groups", "req"), None),
        P(("groups", "req"), None),
        P(("groups", "req"), None, None),
        P(),
        P(),
        P(),
    )
    return jax.shard_map(
        local,
        mesh=mesh,
        in_specs=placed,
        out_specs=(
            P(("groups", "req"), None),
            P(("groups", "req"), None),
            P(("groups", "req"), None, None),
        ),
        check_vma=False,
    )
```
